32 devices in a mesh: dp: 8 (over z, x), mp: 4 (over y, core).
Axes of the slice: x: 2, y: 2, z: 4, core: 2. Of those that a mesh axis runs over, the one named last changes fastest.
Arguments:
- stats: float32 [4, 64, 256, 256], P('mp', 'dp'), may hold values from -1 to 1, as said below
- prev_roots: float32 [4, 64, 256, 256], P('mp', 'dp'), may hold values from -1 to 2, as said below
- counts: int32 [4, 8], replicated, may hold values from 1 to 8, as said below
- grads: bfloat16 [4, 64, 256, 1024], P(None, 'dp', None, 'mp'), may hold values from -6 to 6
Outputs:
- precond: bfloat16 [4, 64, 256, 1024], P(None, 'dp', None, 'mp')
The draws below stay inside these ranges and needn't reach their ends.
Inputs may be any that keep to these rules, and one draw needn't show every extreme that they name: Each model shard's live blocks are the first count slots of each of its devices; every count is 1 to 8, 8 is reached on some device, and the counts of one model shard sum to at most 32, which some model shard reaches. `stats`: every block is symmetric positive definite. `prev_roots`: every block is symmetric.
All inputs are finite; a program needn't handle non-finite values.
Results may differ from the reference program's by a relative error of at most 0.0052.
Values may be sent and summed in bfloat16 or wider, within the bound.
A program may use at most 128 MiB of HBM per device.

```python
import math
import jax
import jax.numpy as jnp
from jax import lax

B = 256
NEWTON = 2
SLOT = 8
SHARE = 4
OWNERS = 4
WORKERS = 8


def symmetric_noise(noise_key, block_shape, spread):
    values = jnp.clip(jax.random.normal(noise_key, block_shape, jnp.float32), -4.0, 4.0)
    return (values + jnp.swapaxes(values, -1, -2)) * (spread / math.sqrt(2.0 * B))


def draw_stats(key, part):
    block_shape = (OWNERS, WORKERS * SLOT, B, B)
    first_key, second_key = jax.random.split(jax.random.fold_in(key, 101))
    noise_part = symmetric_noise(first_key, block_shape, 0.25)
    scales = jnp.exp(jax.random.uniform(second_key, block_shape[:-1], jnp.float32, math.log(0.8), math.log(1.25)))
    identity = jnp.eye(B, dtype=jnp.float32)
    return 0.4 * scales[..., :, None] * (identity + noise_part) * scales[..., None, :]


def draw_prev_roots(key, part):
    block_shape = (OWNERS, WORKERS * SLOT, B, B)
    noise_part = symmetric_noise(jax.random.fold_in(key, 202), block_shape, 0.2)
    return jnp.eye(B, dtype=jnp.float32) + noise_part


def draw_counts(key, part):
    key_list = jax.random.split(jax.random.fold_in(key, 303), 4)
    spare_units = (SHARE - 1) * WORKERS
    full_row = jax.random.randint(key_list[0], (), 0, OWNERS)
    extra_units = jax.random.randint(key_list[1], (OWNERS,), 3 * spare_units // 4, spare_units + 1)
    is_full = jnp.arange(OWNERS) == full_row
    extra_units = jnp.where(is_full, spare_units, extra_units)
    favoured = jax.random.randint(key_list[2], (OWNERS,), 0, WORKERS)
    unit_count = WORKERS * (SLOT - 1)
    scores = jax.random.randint(key_list[3], (OWNERS, WORKERS, SLOT - 1), 0, 65536)
    position = jnp.arange(unit_count, dtype=jnp.int32).reshape(1, WORKERS, SLOT - 1)
    boosted = (jnp.arange(WORKERS)[None, :, None] == favoured[:, None, None]) & is_full[:, None, None]
    scores = scores * unit_count + position + boosted.astype(jnp.int32) * (65536 * unit_count)
    flat_scores = scores.reshape(OWNERS, unit_count)
    ordering = jnp.argsort(-flat_scores, axis=1)
    unit_rank = jnp.argsort(ordering, axis=1)
    chosen = (unit_rank < extra_units[:, None]).astype(jnp.int32).reshape(OWNERS, WORKERS, SLOT - 1)
    return (1 + jnp.sum(chosen, axis=2)).astype(jnp.int32)


def levels(stream_key, extent, shards, least, largest):
    loudness = 1.0
    for axis_at, parts in shards:
        heights = jax.random.uniform(jax.random.fold_in(jax.random.fold_in(stream_key, 6), axis_at), (parts,), jnp.float32, least / len(shards), largest / len(shards))
        loudness = loudness * jnp.repeat(jnp.exp(heights), extent[axis_at] // parts).reshape((-1,) + (1,) * (len(extent) - 1 - axis_at))
    return loudness


def bell_draw(rng, extent, scale, reach, shards=(), kind=jnp.bfloat16):
    values = jax.random.normal(rng, extent, jnp.float32) * scale
    if len(shards) > 0:
        values = levels(rng, extent, shards, -0.22, 0.18) * values
    return jnp.clip(values, min=-reach, max=reach).astype(kind)


def setup_inputs(seed: int = 0) -> dict:
    seeds = jax.random.split(jax.random.key(seed), 5)
    stats = draw_stats(jax.random.fold_in(seeds[4], 71), 0)
    prev_roots = draw_prev_roots(jax.random.fold_in(seeds[4], 71), 0)
    counts = draw_counts(jax.random.fold_in(seeds[4], 71), 0)
    grads = bell_draw(seeds[3], (OWNERS, WORKERS * SLOT, B, OWNERS * B), 1.0, 6.0, ((1, 8), (3, 4)))
    return dict(stats=stats, prev_roots=prev_roots, counts=counts, grads=grads)


def product(left_side, right_side):
    return jnp.einsum("nij,njk->nik", left_side, right_side, precision=lax.Precision.HIGHEST)


def newton_root(statistic, initial):
    identity = jnp.eye(statistic.shape[-1], dtype=statistic.dtype)
    square = product(initial, initial)
    moment = product(product(square, square), statistic)
    estimate = initial
    for iteration in range(NEWTON):
        newton_step = (5.0 * identity - moment) * 0.25
        estimate = product(estimate, newton_step)
        if iteration + 1 < NEWTON:
            double = product(newton_step, newton_step)
            moment = product(product(double, double), moment)
    return estimate


def precondition_owner(paired):
    left_side = paired[0].astype(jnp.float32)
    right_side = paired[1].astype(jnp.float32)
    return jnp.einsum("gab,gbc->gac", left_side, right_side).astype(jnp.bfloat16)


def reference(stats, prev_roots, counts, grads):
    block_groups = OWNERS * WORKERS
    grouped = (stats.reshape(block_groups, SLOT, B, B), prev_roots.reshape(block_groups, SLOT, B, B))
    root_blocks = lax.map(lambda paired: newton_root(paired[0], paired[1]), grouped)
    live_mask = jnp.arange(SLOT, dtype=jnp.int32)[None, None, :] < counts[:, :, None]
    live_mask = live_mask.reshape(block_groups, SLOT, 1, 1)
    band_root = jnp.where(live_mask, root_blocks.astype(jnp.bfloat16), jnp.zeros((), jnp.bfloat16))
    band_root = band_root.reshape(OWNERS, WORKERS * SLOT, B, B)
    return lax.map(precondition_owner, (band_root, grads))
```

```python
import functools

import jax
import jax.numpy as jnp
from jax import lax
from jax.experimental import pallas as pl
from jax.experimental.pallas import tpu as pltpu
from jax.sharding import PartitionSpec as P

NEWTON = 2
MESH = pl.DeviceIdType.MESH


def split(value):
    high = value.astype(jnp.bfloat16)
    return high, (value - high.astype(jnp.float32)).astype(jnp.bfloat16)


def dot(left, right):
    return jnp.dot(left, right, preferred_element_type=jnp.float32)


def product(left, right):
    return dot(left[0], right[0]) + (dot(left[0], right[1]) + dot(left[1], right[0]))


def newton_root(statistic, initial):
    size = initial.shape[-1]
    rows = lax.broadcasted_iota(jnp.int32, (size, size), 0)
    columns = lax.broadcasted_iota(jnp.int32, (size, size), 1)
    identity = jnp.where(rows == columns, 1.25, 0.0).astype(jnp.float32)
    start = split(initial)
    square = split(product(start, start))
    fourth = split(product(square, square))
    moment = product(fourth, split(statistic))
    estimate = start
    for iteration in range(NEWTON):
        step = split(identity - 0.25 * moment)
        result = product(estimate, step)
        if iteration + 1 < NEWTON:
            estimate = split(result)
            double = split(product(step, step))
            moment = product(split(product(double, double)), split(moment))
    return result


def kernel(members, counts, stats, starts, grads, out, a_buf, x_buf, g_buf, roots,
           a_sem, x_sem, g_sem, y_send, y_recv, p_send, p_recv, f_send, f_recv):
    me = lax.axis_index("mp")
    data = lax.axis_index("dp")
    slots = stats.shape[1]
    chips = members // 2
    core = lax.rem(me, 2)
    chip = me // 2
    partner = me + 1 - 2 * core

    def peer(offset, which):
        return lax.rem(chip + offset, chips) * 2 + which

    def a_copy(slot):
        return pltpu.make_async_copy(stats.at[0, slot], a_buf.at[slot], a_sem.at[slot])

    def x_copy(slot):
        return pltpu.make_async_copy(starts.at[0, slot], x_buf.at[slot], x_sem.at[slot])

    def g_copy(owner):
        return pltpu.make_async_copy(grads.at[owner], g_buf.at[owner], g_sem.at[owner])

    def send(owner, slot, target, send_sem, recv_sem):
        return pltpu.make_async_remote_copy(
            src_ref=roots.at[owner, slot], dst_ref=roots.at[owner, slot],
            send_sem=send_sem, recv_sem=recv_sem,
            device_id={"mp": target}, device_id_type=MESH)

    def y_copy(owner, offset, slot):
        return send(owner, slot, peer(offset, core), y_send.at[offset - 1, slot], y_recv.at[offset - 1, slot])

    def p_copy(owner, slot):
        return send(owner, slot, partner, p_send.at[slot], p_recv.at[slot])

    def f_copy(owner, offset, slot):
        return send(owner, slot, partner, f_send.at[offset - 1, slot], f_recv.at[offset - 1, slot])

    for slot in range(slots):
        x_copy(slot).start()
        a_copy(slot).start()
    for owner in range(members):
        g_copy(owner).start()

    barrier = pltpu.get_barrier_semaphore()
    pl.semaphore_signal(barrier, inc=1, device_id={"mp": partner}, device_id_type=MESH)
    for offset in range(1, chips):
        pl.semaphore_signal(barrier, inc=1, device_id={"mp": peer(offset, core)}, device_id_type=MESH)
    pl.semaphore_wait(barrier, chips)

    live_count = counts[me, data]

    @pl.loop(0, slots)
    def _(slot):
        x_copy(slot).wait()
        a_copy(slot).wait()
        root = newton_root(a_buf[slot], x_buf[slot])
        live = jnp.full(root.shape, slot, jnp.int32) < live_count
        roots[me, slot] = jnp.where(live, root, 0.0).astype(jnp.bfloat16)
        for offset in range(1, chips):
            y_copy(me, offset, slot).start()
        p_copy(me, slot).start()

    for owner in range(members):
        g_copy(owner).wait()

    def apply(owner, slot):
        out[owner, slot] = dot(roots[owner, slot], g_buf[owner, slot]).astype(out.dtype)

    @pl.loop(0, slots)
    def _(slot):
        apply(me, slot)
        p_copy(partner, slot).wait_recv()
        apply(partner, slot)

    @pl.loop(0, slots)
    def _(slot):
        for offset in range(1, chips):
            owner = peer(chips - offset, core)
            y_copy(owner, offset, slot).wait_recv()
            f_copy(owner, offset, slot).start()
            apply(owner, slot)
        for offset in range(1, chips):
            owner = peer(chips - offset, 1 - core)
            f_copy(owner, offset, slot).wait_recv()
            apply(owner, slot)

    @pl.loop(0, slots)
    def _(slot):
        p_copy(me, slot).wait_send()
        for offset in range(1, chips):
            y_copy(me, offset, slot).wait_send()
            f_copy(peer(chips - offset, core), offset, slot).wait_send()


def local(members, stats, prev_roots, counts, grads):
    slots, size = stats.shape[1], stats.shape[2]
    chips = members // 2
    block = (slots, size, size)
    return pl.pallas_call(
        functools.partial(kernel, members),
        out_shape=jax.ShapeDtypeStruct(grads.shape, grads.dtype),
        in_specs=[pl.BlockSpec(memory_space=pltpu.SMEM)] + [pl.BlockSpec(memory_space=pl.ANY)] * 3,
        out_specs=pl.BlockSpec(memory_space=pltpu.VMEM),
        scratch_shapes=[
            pltpu.VMEM(block, jnp.float32),
            pltpu.VMEM(block, jnp.float32),
            pltpu.VMEM(grads.shape, grads.dtype),
            pltpu.VMEM((members,) + block, jnp.bfloat16),
            pltpu.SemaphoreType.DMA((slots,)),
            pltpu.SemaphoreType.DMA((slots,)),
            pltpu.SemaphoreType.DMA((members,)),
            pltpu.SemaphoreType.DMA((chips - 1, slots)),
            pltpu.SemaphoreType.DMA((chips - 1, slots)),
            pltpu.SemaphoreType.DMA((slots,)),
            pltpu.SemaphoreType.DMA((slots,)),
            pltpu.SemaphoreType.DMA((chips - 1, slots)),
            pltpu.SemaphoreType.DMA((chips - 1, slots)),
        ],
        compiler_params=pltpu.CompilerParams(
            collective_id=0, has_side_effects=True, vmem_limit_bytes=56 * 1024 * 1024),
    )(counts, stats, prev_roots, grads)


def solution(mesh):
    return jax.shard_map(
        functools.partial(local, mesh.shape["mp"]),
        mesh=mesh,
        in_specs=(
            P("mp", "dp", None, None),
            P("mp", "dp", None, None),
            P(),
            P(None, "dp", None, "mp"),
        ),
        out_specs=P(None, "dp", None, "mp"),
        check_vma=False,
    )
```

```python
import functools

import jax
import jax.numpy as jnp
from jax import lax
from jax.experimental import pallas as pl
from jax.experimental.pallas import tpu as pltpu
from jax.sharding import PartitionSpec as P

NEWTON = 2
VMEM_BYTES = 67043328 - 65536
MESH = pl.DeviceIdType.MESH


def dot(left, right):
    return jnp.dot(left.astype(jnp.bfloat16), right.astype(jnp.bfloat16), preferred_element_type=jnp.float32)


def shifted_square(part):
    return 2.0 * part + dot(part, part)


def newton_root(statistic, initial):
    size = initial.shape[-1]
    rows = lax.broadcasted_iota(jnp.int32, (size, size), 0)
    columns = lax.broadcasted_iota(jnp.int32, (size, size), 1)
    identity = jnp.where(rows == columns, 1.0, 0.0).astype(jnp.float32)
    moment = statistic + dot(shifted_square(shifted_square(initial - identity)), statistic)
    estimate = initial
    for iteration in range(NEWTON):
        change = 0.25 * (identity - moment)
        estimate = estimate + dot(estimate, change)
        if iteration + 1 < NEWTON:
            moment = moment + dot(shifted_square(shifted_square(change)), moment)
    return estimate


def kernel(members, count_table, stats, starts, grads, out, counts, count_sem, a_buf, x_buf, g_buf, roots,
           a_sem, x_sem, g_sem, y_send, y_recv, p_send, p_recv, f_send, f_recv):
    me = lax.axis_index("mp")
    data = lax.axis_index("dp")
    slots = stats.shape[1]
    chips = members // 2
    core = lax.rem(me, 2)
    chip = me // 2
    partner = me + 1 - 2 * core

    def peer(offset, which):
        return lax.rem(chip + offset, chips) * 2 + which

    def a_copy(slot):
        return pltpu.make_async_copy(stats.at[0, slot], a_buf.at[slot], a_sem.at[slot])

    def x_copy(slot):
        return pltpu.make_async_copy(starts.at[0, slot], x_buf.at[slot], x_sem.at[slot])

    def g_copy(owner):
        return pltpu.make_async_copy(grads.at[owner], g_buf.at[owner], g_sem.at[owner])

    def send(owner, slot, target, send_sem, recv_sem):
        return pltpu.make_async_remote_copy(
            src_ref=roots.at[owner, slot], dst_ref=roots.at[owner, slot],
            send_sem=send_sem, recv_sem=recv_sem,
            device_id={"mp": target}, device_id_type=MESH)

    def y_copy(owner, offset, slot):
        return send(owner, slot, peer(offset, core), y_send.at[offset - 1, slot], y_recv.at[offset - 1, slot])

    def p_copy(owner, slot):
        return send(owner, slot, partner, p_send.at[slot], p_recv.at[slot])

    def f_copy(owner, offset, slot):
        return send(owner, slot, partner, f_send.at[offset - 1, slot], f_recv.at[offset - 1, slot])

    count_copy = pltpu.make_async_copy(count_table, counts, count_sem)
    count_copy.start()
    for slot in range(slots):
        x_copy(slot).start()
        a_copy(slot).start()
    for owner in range(members):
        g_copy(owner).start()

    barrier = pltpu.get_barrier_semaphore()
    pl.semaphore_signal(barrier, inc=1, device_id={"mp": partner}, device_id_type=MESH)
    for offset in range(1, chips):
        pl.semaphore_signal(barrier, inc=1, device_id={"mp": peer(offset, core)}, device_id_type=MESH)
    pl.semaphore_wait(barrier, chips)

    count_copy.wait()
    live_count = counts[me, data]

    @pl.loop(0, slots)
    def _(slot):
        x_copy(slot).wait()
        a_copy(slot).wait()
        root = newton_root(a_buf[slot], x_buf[slot])
        live = jnp.full(root.shape, slot, jnp.int32) < live_count
        roots[me, slot] = jnp.where(live, root, 0.0).astype(jnp.bfloat16)
        for offset in range(1, chips):
            y_copy(me, offset, slot).start()
        p_copy(me, slot).start()

    for owner in range(members):
        g_copy(owner).wait()

    def apply(owner, slot):
        out[owner, slot] = dot(roots[owner, slot], g_buf[owner, slot]).astype(out.dtype)

    @pl.loop(0, slots)
    def _(slot):
        apply(me, slot)
        p_copy(partner, slot).wait_recv()
        apply(partner, slot)

    @pl.loop(0, slots)
    def _(slot):
        for offset in range(1, chips):
            owner = peer(chips - offset, core)
            y_copy(owner, offset, slot).wait_recv()
            f_copy(owner, offset, slot).start()
            apply(owner, slot)
        for offset in range(1, chips):
            owner = peer(chips - offset, 1 - core)
            f_copy(owner, offset, slot).wait_recv()
            apply(owner, slot)

    @pl.loop(0, slots)
    def _(slot):
        p_copy(me, slot).wait_send()
        for offset in range(1, chips):
            y_copy(me, offset, slot).wait_send()
            f_copy(peer(chips - offset, core), offset, slot).wait_send()


def local(members, stats, prev_roots, counts, grads):
    slots, size = stats.shape[1], stats.shape[2]
    chips = members // 2
    block = (slots, size, size)
    out_bytes = grads.size * grads.dtype.itemsize
    return pl.pallas_call(
        functools.partial(kernel, members),
        out_shape=pltpu.VMEM(grads.shape, grads.dtype),
        in_specs=[pl.BlockSpec(memory_space=pltpu.HBM)] * 4,
        out_specs=pl.BlockSpec(memory_space=pltpu.VMEM),
        scratch_shapes=[
            pltpu.SMEM(counts.shape, counts.dtype),
            pltpu.SemaphoreType.DMA,
            pltpu.VMEM(block, jnp.float32),
            pltpu.VMEM(block, jnp.float32),
            pltpu.VMEM(grads.shape, grads.dtype),
            pltpu.VMEM((members,) + block, jnp.bfloat16),
            pltpu.SemaphoreType.DMA((slots,)),
            pltpu.SemaphoreType.DMA((slots,)),
            pltpu.SemaphoreType.DMA((members,)),
            pltpu.SemaphoreType.DMA((chips - 1, slots)),
            pltpu.SemaphoreType.DMA((chips - 1, slots)),
            pltpu.SemaphoreType.DMA((slots,)),
            pltpu.SemaphoreType.DMA((slots,)),
            pltpu.SemaphoreType.DMA((chips - 1, slots)),
            pltpu.SemaphoreType.DMA((chips - 1, slots)),
        ],
        compiler_params=pltpu.CompilerParams(
            collective_id=0, has_side_effects=True, vmem_limit_bytes=VMEM_BYTES - out_bytes),
    )(counts, stats, prev_roots, grads)


def solution(mesh):
    return jax.shard_map(
        functools.partial(local, mesh.shape["mp"]),
        mesh=mesh,
        in_specs=(
            P("mp", "dp", None, None),
            P("mp", "dp", None, None),
            P(),
            P(None, "dp", None, "mp"),
        ),
        out_specs=P(None, "dp", None, "mp"),
        check_vma=False,
    )
```

```python
import functools

import jax
import jax.numpy as jnp
from jax import lax
from jax.experimental import pallas as pl
from jax.experimental.pallas import tpu as pltpu
from jax.sharding import PartitionSpec as P

NEWTON = 2
PIECES = 1
VMEM_BYTES = 67043328 - 65536
MESH = pl.DeviceIdType.MESH


def dot(left, right):
    return jnp.dot(left.astype(jnp.bfloat16), right.astype(jnp.bfloat16), preferred_element_type=jnp.float32)


def shifted_square(part):
    return 2.0 * part + dot(part, part)


def newton_root(statistic, initial):
    size = initial.shape[-1]
    rows = lax.broadcasted_iota(jnp.int32, (size, size), 0)
    columns = lax.broadcasted_iota(jnp.int32, (size, size), 1)
    identity = jnp.where(rows == columns, 1.0, 0.0).astype(jnp.float32)
    moment = statistic + dot(shifted_square(shifted_square(initial - identity)), statistic)
    estimate = initial
    for iteration in range(NEWTON):
        change = 0.25 * (identity - moment)
        estimate = estimate + dot(estimate, change)
        if iteration + 1 < NEWTON:
            moment = moment + dot(shifted_square(shifted_square(change)), moment)
    return estimate


def kernel(members, count_table, stats, starts, grads, out, counts, count_sem, a_buf, x_buf, g_buf, roots,
           a_sem, x_sem, g_sem, y_send, y_recv, p_send, p_recv, f_send, f_recv):
    me = lax.axis_index("mp")
    data = lax.axis_index("dp")
    slots = stats.shape[1]
    chips = members // 2
    core = lax.rem(me, 2)
    chip = me // 2
    partner = me + 1 - 2 * core

    def peer(offset, which):
        return lax.rem(chip + offset, chips) * 2 + which

    def a_copy(slot):
        return pltpu.make_async_copy(stats.at[0, slot], a_buf.at[slot], a_sem.at[slot])

    def x_copy(slot):
        return pltpu.make_async_copy(starts.at[0, slot], x_buf.at[slot], x_sem.at[slot])

    def g_copy(owner):
        return pltpu.make_async_copy(grads.at[owner], g_buf.at[owner], g_sem.at[owner])

    def send(block, target, send_sem, recv_sem):
        return pltpu.make_async_remote_copy(
            src_ref=block, dst_ref=block, send_sem=send_sem, recv_sem=recv_sem,
            device_id={"mp": target}, device_id_type=MESH)

    height = roots.shape[2] // PIECES

    def strip(piece):
        return pl.ds(pl.multiple_of(piece * height, height), height)

    def y_copy(owner, offset, slot, piece):
        at = offset - 1, slot, piece
        return send(roots.at[owner, slot, strip(piece)], peer(offset, core), y_send.at[at], y_recv.at[at])

    def p_copy(owner, slot):
        return send(roots.at[owner, slot], partner, p_send.at[slot], p_recv.at[slot])

    def f_copy(owner, offset, slot, piece):
        at = offset - 1, slot, piece
        return send(roots.at[owner, slot, strip(piece)], partner, f_send.at[at], f_recv.at[at])

    count_copy = pltpu.make_async_copy(count_table, counts, count_sem)
    x_copy(0).start()
    a_copy(0).start()
    count_copy.start()

    barrier = pltpu.get_barrier_semaphore()
    pl.semaphore_signal(barrier, inc=1, device_id={"mp": partner}, device_id_type=MESH)
    for offset in range(1, chips):
        pl.semaphore_signal(barrier, inc=1, device_id={"mp": peer(offset, core)}, device_id_type=MESH)

    count_copy.wait()
    live_count = counts[me, data]

    def compute(slot):
        root = newton_root(a_buf[slot], x_buf[slot])
        live = jnp.full(root.shape, slot, jnp.int32) < live_count
        roots[me, slot] = jnp.where(live, root, 0.0).astype(jnp.bfloat16)

    def launch(slot):
        for piece in range(PIECES):
            for offset in range(1, chips):
                y_copy(me, offset, slot, piece).start()
        p_copy(me, slot).start()

    x_copy(0).wait()
    a_copy(0).wait()
    for slot in range(1, slots):
        x_copy(slot).start()
        a_copy(slot).start()
    for owner in range(members):
        g_copy(owner).start()
    compute(0)
    pl.semaphore_wait(barrier, chips)
    launch(0)

    @pl.loop(1, slots)
    def _(slot):
        x_copy(slot).wait()
        a_copy(slot).wait()
        compute(slot)
        launch(slot)

    for owner in range(members):
        g_copy(owner).wait()

    def apply(owner, slot):
        out[owner, slot] = dot(roots[owner, slot], g_buf[owner, slot]).astype(out.dtype)

    @pl.loop(0, slots)
    def _(slot):
        apply(me, slot)
        p_copy(partner, slot).wait_recv()
        apply(partner, slot)

    def apply_strip(owner, slot, piece):
        part = strip(piece)
        out[owner, slot, part] = dot(roots[owner, slot, part], g_buf[owner, slot]).astype(out.dtype)

    def arrive(count):
        slot, piece = count // PIECES, lax.rem(count, PIECES)
        for offset in range(1, chips):
            owner = peer(chips - offset, core)
            y_copy(owner, offset, slot, piece).wait_recv()
            f_copy(owner, offset, slot, piece).start()
            apply_strip(owner, slot, piece)

    def passed(count):
        slot, piece = count // PIECES, lax.rem(count, PIECES)
        for offset in range(1, chips):
            owner = peer(chips - offset, 1 - core)
            f_copy(owner, offset, slot, piece).wait_recv()
            apply_strip(owner, slot, piece)

    arrive(jnp.int32(0))

    @pl.loop(1, slots * PIECES)
    def _(count):
        arrive(count)
        passed(count - 1)

    passed(jnp.int32(slots * PIECES - 1))

    @pl.loop(0, slots)
    def _(slot):
        p_copy(me, slot).wait_send()
        for piece in range(PIECES):
            for offset in range(1, chips):
                y_copy(me, offset, slot, piece).wait_send()
                f_copy(peer(chips - offset, core), offset, slot, piece).wait_send()


def local(members, stats, prev_roots, counts, grads):
    slots, size = stats.shape[1], stats.shape[2]
    chips = members // 2
    block = (slots, size, size)
    out_bytes = grads.size * grads.dtype.itemsize
    return pl.pallas_call(
        functools.partial(kernel, members),
        out_shape=pltpu.VMEM(grads.shape, grads.dtype),
        in_specs=[pl.BlockSpec(memory_space=pltpu.HBM)] * 4,
        out_specs=pl.BlockSpec(memory_space=pltpu.VMEM),
        scratch_shapes=[
            pltpu.SMEM(counts.shape, counts.dtype),
            pltpu.SemaphoreType.DMA,
            pltpu.VMEM(block, jnp.float32),
            pltpu.VMEM(block, jnp.float32),
            pltpu.VMEM(grads.shape, grads.dtype),
            pltpu.VMEM((members,) + block, jnp.bfloat16),
            pltpu.SemaphoreType.DMA((slots,)),
            pltpu.SemaphoreType.DMA((slots,)),
            pltpu.SemaphoreType.DMA((members,)),
            pltpu.SemaphoreType.DMA((chips - 1, slots, PIECES)),
            pltpu.SemaphoreType.DMA((chips - 1, slots, PIECES)),
            pltpu.SemaphoreType.DMA((slots,)),
            pltpu.SemaphoreType.DMA((slots,)),
            pltpu.SemaphoreType.DMA((chips - 1, slots, PIECES)),
            pltpu.SemaphoreType.DMA((chips - 1, slots, PIECES)),
        ],
        compiler_params=pltpu.CompilerParams(
            collective_id=0, has_side_effects=True, vmem_limit_bytes=VMEM_BYTES - out_bytes),
    )(counts, stats, prev_roots, grads)


def solution(mesh):
    return jax.shard_map(
        functools.partial(local, mesh.shape["mp"]),
        mesh=mesh,
        in_specs=(
            P("mp", "dp", None, None),
            P("mp", "dp", None, None),
            P(),
            P(None, "dp", None, "mp"),
        ),
        out_specs=P(None, "dp", None, "mp"),
        check_vma=False,
    )
```
